32 devices in a mesh: row: 4 (over y, x), col: 8 (over z, core).
Axes of the slice: x: 2, y: 2, z: 4, core: 2. Of those that a mesh axis runs over, the one named last changes fastest.
Arguments:
- features: bfloat16 [32768, 128], P(('row', 'col')), may hold values from -24 to 24
- tile_rows: int32 [4, 8, 1024], P('row', 'col'), may hold values from 0 to 63
- tile_cols: int32 [4, 8, 1024], P('row', 'col'), may hold values from 0 to 31
- edge_lists: int32 [2, 4, 8, 1024, 128], P(None, 'row', 'col'), may hold values from -16 to 127
- tile_counts: int32 [4, 8], P('row', 'col'), may hold values from 128 to 1024, as said below
Outputs:
- hop_one: bfloat16 [32768, 128], P(('row', 'col'))
- hop_two: bfloat16 [32768, 128], P(('row', 'col'))
The draws below stay inside these ranges and needn't reach their ends.
Inputs may be any that keep to these rules, and one draw needn't show every extreme that they name: `tile_counts`: live tile slots of a block; some block has exactly 1024. `edge_lists`: a negative entry marks an empty edge slot; slots at or past a block's count hold arbitrary entries. `tile_rows`: a tile may occur in several slots; slots at or past a block's count hold arbitrary entries. `tile_cols`: slots at or past a block's count hold arbitrary entries.
All inputs are finite; a program needn't handle non-finite values.
Results may differ from the reference program's by a relative error of at most 0.0058.
Values may be sent and summed in bfloat16 or wider, within the bound.
A program may use at most 192 MiB of HBM per device.

```python
import jax
import jax.numpy as jnp
from jax import lax

F = 128
TILE = 128
EDGE_TILE = 128
NODE_DEV = 1024
TILE_MOST = 1024
NODES = 32768
TILE_ROWS = 64
TILE_COLS = 32
N_ROW = 4
N_COL = 8


def draw_tile_counts(key, part):
    base = jax.random.randint(jax.random.fold_in(key, 11), (N_ROW * N_COL,), TILE_MOST // 8, TILE_MOST // 2 + 1)
    busiest = jax.random.randint(jax.random.fold_in(key, 12), (), 0, N_ROW * N_COL)
    placed = jnp.where(jnp.arange(N_ROW * N_COL) == busiest, TILE_MOST, base)
    return placed.reshape(N_ROW, N_COL).astype(jnp.int32)


def set_ends(result, key, smallest, high):
    shape = result.shape
    place = [jax.random.randint(jax.random.fold_in(key, axis), (), 0, shape[axis]) for axis in range(len(shape))]
    result = result.at[tuple(place)].set(smallest)
    longest = shape.index(max(shape))
    place[longest] = (place[longest] + 1) % shape[longest]
    return result.at[tuple(place)].set(high)


def level_of(key, dims, shards, low, largest):
    factor_of, own = 1.0, jax.random.fold_in(key, 6)
    for dim, shards_of in shards:
        steps = jnp.exp(jax.random.uniform(jax.random.fold_in(own, dim), (shards_of,), jnp.float32, low / len(shards), largest / len(shards)))
        factor_of = factor_of * jnp.repeat(steps, dims[dim] // shards_of).reshape([-1 if axis == dim else 1 for axis in range(len(dims))])
    return factor_of


def scatter_about(rng, shape, scale, bound, shards=(), dtype=jnp.bfloat16):
    values = scale * jax.random.normal(rng, shape, jnp.float32)
    if shards:
        values = values * level_of(rng, shape, shards, -0.22, 0.18)
    return jnp.clip(values, -bound, bound).astype(dtype)


def setup_inputs(seed: int = 0) -> dict:
    keys = jax.random.split(jax.random.key(seed), 6)
    features = scatter_about(keys[0], (NODES, F), 4.0, 24.0, ((0, 32),))
    tile_rows = set_ends(jax.random.randint(keys[1], (N_ROW, N_COL, TILE_MOST), 0, TILE_ROWS), jax.random.fold_in(keys[1], 1), 0, TILE_ROWS - 1).astype(jnp.int32)
    tile_cols = set_ends(jax.random.randint(keys[2], (N_ROW, N_COL, TILE_MOST), 0, TILE_COLS), jax.random.fold_in(keys[2], 1), 0, TILE_COLS - 1).astype(jnp.int32)
    edge_lists = set_ends(jax.random.randint(keys[3], (2, N_ROW, N_COL, TILE_MOST, EDGE_TILE), -16, TILE), jax.random.fold_in(keys[3], 1), -16, TILE - 1).astype(jnp.int32)
    tile_counts = draw_tile_counts(jax.random.fold_in(keys[5], 71), 0)
    return dict(features=features, tile_rows=tile_rows, tile_cols=tile_cols, edge_lists=edge_lists, tile_counts=tile_counts)


def reference(features, tile_rows, tile_cols, edge_lists, tile_counts):
    node_total = NODE_DEV * N_ROW * N_COL
    block_nodes = NODE_DEV * N_COL
    slot_ids = lax.iota(jnp.int32, TILE_MOST)

    def edges_of(device_idx):
        row_idx = device_idx // N_COL
        col_idx = device_idx % N_COL
        dst_ids = edge_lists[0, row_idx, col_idx]
        src_ids = edge_lists[1, row_idx, col_idx]
        alive = (slot_ids < tile_counts[row_idx, col_idx])[:, None] & (dst_ids >= 0) & (src_ids >= 0)
        target = row_idx * block_nodes + tile_rows[row_idx, col_idx][:, None] * TILE + dst_ids
        column = tile_cols[row_idx, col_idx][:, None] * TILE + src_ids
        source = (column // NODE_DEV * N_COL + col_idx) * NODE_DEV + column % NODE_DEV
        target = jnp.where(alive, target, 0).reshape(-1)
        source = jnp.where(alive, source, 0).reshape(-1)
        return (target, source, alive.astype(jnp.float32).reshape(-1))

    def count_edges(device_idx, degree):
        target, source, weight = edges_of(device_idx)
        return degree.at[target].add(weight)
    degree = lax.fori_loop(0, N_ROW * N_COL, count_edges, jnp.zeros((node_total,), jnp.float32))
    inv_root = lax.rsqrt(1.0 + degree)

    def propagate(scaled):

        def add_edges(device_idx, summed):
            target, source, weight = edges_of(device_idx)
            return summed.at[target].add(scaled[source].astype(jnp.float32) * weight[:, None])
        return lax.fori_loop(0, N_ROW * N_COL, add_edges, jnp.zeros((node_total, F), jnp.float32))
    scaled_zero = (features.astype(jnp.float32) * inv_root[:, None]).astype(jnp.bfloat16)
    first_sum = propagate(scaled_zero)
    hop_one = (first_sum * inv_root[:, None]).astype(jnp.bfloat16)
    scaled_one = (first_sum * (inv_root * inv_root)[:, None]).astype(jnp.bfloat16)
    second_sum = propagate(scaled_one)
    hop_two = (second_sum * inv_root[:, None]).astype(jnp.bfloat16)
    return (hop_one, hop_two)
```

```python
import functools

import jax
import jax.numpy as jnp
from jax import lax
from jax.experimental import pallas as pl
from jax.experimental.pallas import tpu as pltpu
from jax.sharding import PartitionSpec as P

TILE = 128
GROUP = 64
UNROLL = 8
EXTRA = 16
PIECES = 4
CORES = 2
MESH_ID = pl.DeviceIdType.MESH
VMEM_SPEC = pl.BlockSpec(memory_space=pltpu.VMEM)


def live_groups(count_ref):
    first = pl.program_id(0) * GROUP
    live = jnp.clip(count_ref[0] - first, 0, GROUP)
    return first, (live + UNROLL - 1) // UNROLL


def build_kernel(count_ref, rows_ref, dst_ref, src_ref, store_ref, degree_ref, degree_acc):
    @pl.when(pl.program_id(0) == 0)
    def _():
        degree_acc[...] = jnp.zeros_like(degree_acc)

    first, turns = live_groups(count_ref)
    cells = lax.broadcasted_iota(jnp.int32, (TILE, TILE), 0)

    def visit(turn, carry):
        for step in range(UNROLL):
            slot = turn * UNROLL + step
            alive = first + slot < count_ref[0]
            row = jnp.where(alive, rows_ref[first + slot], 0)
            dst = jnp.where(alive, dst_ref[pl.ds(slot, 1), :], -1)
            src = src_ref[pl.ds(slot, 1), :]
            dst_hot = jnp.where(dst == cells, 1.0, 0.0).astype(jnp.bfloat16)
            src_hot = jnp.where(src == cells, 1.0, 0.0).astype(jnp.bfloat16)
            valid = jnp.broadcast_to(jnp.where(src >= 0, 1.0, 0.0), (EXTRA, TILE))
            left = jnp.concatenate([src_hot, valid.astype(jnp.bfloat16)], axis=0)
            both = lax.dot_general(
                left, dst_hot, (((1,), (1,)), ((), ())), preferred_element_type=jnp.float32
            )
            store_ref[slot] = both[:TILE].astype(jnp.bfloat16)
            degree_acc[row] += both[TILE : TILE + 8]
        return carry

    lax.fori_loop(0, turns, visit, 0)

    @pl.when(pl.program_id(0) == pl.num_programs(0) - 1)
    def _():
        degree_ref[...] = degree_acc[:, 0, :]


def apply_kernel(count_ref, rows_ref, cols_ref, store_ref, source_ref, out_ref, acc):
    @pl.when(pl.program_id(0) == 0)
    def _():
        acc[...] = jnp.zeros_like(acc)

    first, turns = live_groups(count_ref)

    def visit(turn, carry):
        products = []
        places = []
        for step in range(UNROLL):
            slot = turn * UNROLL + step
            alive = first + slot < count_ref[0]
            places.append(jnp.where(alive, rows_ref[first + slot], 0))
            col = jnp.where(alive, cols_ref[first + slot], 0)
            product = jnp.dot(
                source_ref[col], store_ref[slot], preferred_element_type=jnp.float32
            )
            acc[places[-1]] += product
        return carry

    lax.fori_loop(0, turns, visit, 0)

    @pl.when(pl.program_id(0) == pl.num_programs(0) - 1)
    def _():
        out_ref[...] = acc[...].astype(jnp.bfloat16)


def greet(targets):
    barrier = pltpu.get_barrier_semaphore()
    for target in targets:
        pl.semaphore_signal(barrier, inc=1, device_id=target, device_id_type=MESH_ID)
    pl.semaphore_wait(barrier, len(targets))


def row_peers(n_row):
    row, col = lax.axis_index("row"), lax.axis_index("col")
    return [(lax.rem(row + d, n_row), col) for d in range(1, n_row)]


def sibling_peers(n_col):
    row, col = lax.axis_index("row"), lax.axis_index("col")
    return [(row, lax.rem(col + CORES * d, n_col)) for d in range(1, n_col // CORES)]


def send(src, dst, send_sem, recv_sem, target):
    copy = pltpu.make_async_remote_copy(
        src_ref=src,
        dst_ref=dst,
        send_sem=send_sem,
        recv_sem=recv_sem,
        device_id=target,
        device_id_type=MESH_ID,
    )
    copy.start()
    return copy


def spread_rows(gathered_ref, start, size, sems, n_row, piece):
    send_sem, recv_sem = sems
    copies = []
    for d, target in enumerate(row_peers(n_row)):
        place = gathered_ref.at[pl.ds(start, size)]
        copies.append(send(place, place, send_sem.at[piece, d], recv_sem.at[piece, d], target))
    return copies


def start_kernel(
    n_row, n_col, part_ref, features_ref, gathered_ref, root_ref, taken, deg_send, deg_recv, row_send, row_recv
):
    row, col = lax.axis_index("row"), lax.axis_index("col")
    own = root_ref.shape[0]
    col_targets = [(row, lax.rem(col + d, n_col)) for d in range(1, n_col)]
    greet(col_targets + row_peers(n_row))
    copies = []
    for d, target in enumerate(col_targets):
        copies.append(
            send(
                part_ref.at[pl.ds(target[1] * own, own)],
                taken.at[d],
                deg_send.at[d],
                deg_recv.at[d],
                target,
            )
        )
    degree = part_ref[pl.ds(pl.multiple_of(col * own, own), own), :]
    for d, copy in enumerate(copies):
        copy.wait_recv()
        degree = degree + taken[d]
    root = lax.rsqrt(1.0 + degree)
    root_ref[...] = root
    size = own // PIECES
    for piece in range(PIECES):
        for tile in range(piece * size, (piece + 1) * size):
            block = features_ref[tile * TILE : (tile + 1) * TILE, :].astype(jnp.float32).T
            gathered_ref[row * own + tile] = (block * root[tile : tile + 1, :]).astype(jnp.bfloat16)
        copies += spread_rows(
            gathered_ref, row * own + piece * size, size, (row_send, row_recv), n_row, piece
        )
    for copy in copies[n_col - 1 :]:
        copy.wait_recv()
    for copy in copies:
        copy.wait_send()


def sum_kernel(n_row, n_col, spread, part_ref, root_ref, *refs):
    if spread:
        hop_ref, gathered_ref, near, staged, far, *sems = refs
        near_send, near_recv, far_send, far_recv, row_send, row_recv = sems
    else:
        hop_ref, near, staged, far, near_send, near_recv, far_send, far_recv = refs
    row, col = lax.axis_index("row"), lax.axis_index("col")
    core = lax.rem(col, CORES)
    chip = col // CORES
    n_chip = n_col // CORES
    partner = (row, chip * CORES + 1 - core)
    siblings = sibling_peers(n_col)
    greet([partner] + siblings + (row_peers(n_row) if spread else []))
    own = root_ref.shape[0]
    size = own // PIECES
    near_copies = {}
    for piece in range(PIECES):
        for d in list(range(1, n_chip)) + [0]:
            other = lax.rem(chip + d, n_chip)
            start = (other * CORES + 1 - core) * own + piece * size
            near_copies[piece, d] = send(
                part_ref.at[pl.ds(start, size)],
                near.at[piece, d],
                near_send.at[piece, d],
                near_recv.at[piece, d],
                partner,
            )
    far_copies = {}
    for piece in range(PIECES):
        for d in range(1, n_chip):
            other = lax.rem(chip + d, n_chip)
            near_copies[piece, d].wait_recv()
            start = (other * CORES + core) * own + piece * size
            staged[piece, d - 1] = (
                part_ref[pl.ds(start, size)].astype(jnp.float32)
                + near[piece, d].astype(jnp.float32)
            ).astype(jnp.bfloat16)
            far_copies[piece, d] = send(
                staged.at[piece, d - 1],
                far.at[piece, d - 1],
                far_send.at[piece, d - 1],
                far_recv.at[piece, d - 1],
                siblings[d - 1],
            )
    row_copies = []
    for piece in range(PIECES):
        near_copies[piece, 0].wait_recv()
        start = (chip * CORES + core) * own + piece * size
        total = part_ref[pl.ds(start, size)].astype(jnp.float32) + near[piece, 0].astype(
            jnp.float32
        )
        for d in range(1, n_chip):
            far_copies[piece, d].wait_recv()
            total = total + far[piece, d - 1].astype(jnp.float32)
        roots = [root_ref[piece * size + tile : piece * size + tile + 1, :] for tile in range(size)]
        if spread:
            for tile in range(size):
                gathered_ref[row * own + piece * size + tile] = (
                    total[tile] * (roots[tile] * roots[tile])
                ).astype(jnp.bfloat16)
            row_copies += spread_rows(
                gathered_ref, row * own + piece * size, size, (row_send, row_recv), n_row, piece
            )
        for tile in range(size):
            place = (piece * size + tile) * TILE
            hop_ref[place : place + TILE, :] = (total[tile] * roots[tile]).T.astype(jnp.bfloat16)
    for copy in row_copies:
        copy.wait_recv()
    for copy in list(near_copies.values()) + list(far_copies.values()) + row_copies:
        copy.wait_send()


def sems(*shape):
    return pltpu.SemaphoreType.DMA(shape)


def comm_params(ident):
    return pltpu.CompilerParams(
        collective_id=ident, has_side_effects=True, vmem_limit_bytes=48 * 2**20
    )


def local(features, tile_rows, tile_cols, edge_lists, tile_counts):
    node_count, feat_width = features.shape
    n_row, n_col = lax.axis_size("row"), lax.axis_size("col")
    own = node_count // TILE
    block_tiles = own * n_col
    source_tiles = own * n_row
    slots = tile_rows.shape[-1]
    rows_own = tile_rows[0, 0]
    cols_own = tile_cols[0, 0]
    count = tile_counts[0]
    bf16, f32 = jnp.bfloat16, jnp.float32

    def last_live(turn, count_ref):
        return jnp.minimum(turn, (jnp.maximum(count_ref[0], 1) - 1) // GROUP)

    store, degree = pl.pallas_call(
        build_kernel,
        grid_spec=pltpu.PrefetchScalarGridSpec(
            num_scalar_prefetch=2,
            grid=(slots // GROUP,),
            in_specs=[
                pl.BlockSpec(
                    (None, None, None, GROUP, TILE),
                    lambda i, n, r, side=side: (side, 0, 0, last_live(i, n), 0),
                )
                for side in range(2)
            ],
            out_specs=[
                pl.BlockSpec((GROUP, TILE, TILE), lambda i, n, r: (last_live(i, n), 0, 0)),
                pl.BlockSpec((block_tiles, TILE), lambda i, n, r: (0, 0)),
            ],
            scratch_shapes=[pltpu.VMEM((block_tiles, 8, TILE), f32)],
        ),
        out_shape=[
            jax.ShapeDtypeStruct((slots, TILE, TILE), bf16),
            jax.ShapeDtypeStruct((block_tiles, TILE), f32),
        ],
        name="build",
    )(count, rows_own, edge_lists, edge_lists)

    gathered_type = jax.ShapeDtypeStruct((source_tiles, feat_width, TILE), bf16)
    gathered, root = pl.pallas_call(
        functools.partial(start_kernel, n_row, n_col),
        out_shape=[gathered_type, jax.ShapeDtypeStruct((own, TILE), f32)],
        in_specs=[VMEM_SPEC] * 2,
        out_specs=[VMEM_SPEC] * 2,
        scratch_shapes=[
            pltpu.VMEM((n_col - 1, own, TILE), f32),
            sems(n_col - 1),
            sems(n_col - 1),
            sems(PIECES, n_row - 1),
            sems(PIECES, n_row - 1),
        ],
        compiler_params=comm_params(0),
        name="start",
    )(degree, features)

    def apply(sources):
        return pl.pallas_call(
            apply_kernel,
            grid_spec=pltpu.PrefetchScalarGridSpec(
                num_scalar_prefetch=3,
                grid=(slots // GROUP,),
                in_specs=[
                    pl.BlockSpec((GROUP, TILE, TILE), lambda i, n, r, c: (last_live(i, n), 0, 0)),
                    pl.BlockSpec((source_tiles, feat_width, TILE), lambda i, n, r, c: (0, 0, 0)),
                ],
                out_specs=pl.BlockSpec((block_tiles, feat_width, TILE), lambda i, n, r, c: (0, 0, 0)),
                scratch_shapes=[pltpu.VMEM((block_tiles, feat_width, TILE), f32)],
            ),
            out_shape=jax.ShapeDtypeStruct((block_tiles, feat_width, TILE), bf16),
            compiler_params=pltpu.CompilerParams(vmem_limit_bytes=48 * 2**20),
            name="apply",
        )(count, rows_own, cols_own, store, sources)

    def collect(part, spread):
        n_chip = n_col // CORES
        size = own // PIECES
        outs = [jax.ShapeDtypeStruct((node_count, feat_width), bf16)]
        semaphores = [sems(PIECES, n_chip)] * 2 + [sems(PIECES, n_chip - 1)] * 2
        if spread:
            outs.append(gathered_type)
            semaphores += [sems(PIECES, n_row - 1)] * 2
        return pl.pallas_call(
            functools.partial(sum_kernel, n_row, n_col, spread),
            out_shape=outs,
            in_specs=[VMEM_SPEC] * 2,
            out_specs=[VMEM_SPEC] * len(outs),
            scratch_shapes=[
                pltpu.VMEM((PIECES, n_chip, size, feat_width, TILE), bf16),
                pltpu.VMEM((PIECES, n_chip - 1, size, feat_width, TILE), bf16),
                pltpu.VMEM((PIECES, n_chip - 1, size, feat_width, TILE), bf16),
            ]
            + semaphores,
            compiler_params=comm_params(1 if spread else 2),
            name="spread" if spread else "finish",
        )(part, root)

    hop_one, gathered = collect(apply(gathered), True)
    (hop_two,) = collect(apply(gathered), False)
    return (hop_one, hop_two)


def solution(mesh):
    placed = (
        P(("row", "col"), None),
        P("row", "col", None),
        P("row", "col", None),
        P(None, "row", "col", None, None),
        P("row", "col"),
    )
    return jax.shard_map(
        local,
        mesh=mesh,
        in_specs=placed,
        out_specs=(P(("row", "col"), None), P(("row", "col"), None)),
        check_vma=False,
    )
```

```python
import functools

import jax
import jax.numpy as jnp
from jax import lax
from jax.experimental import pallas as pl
from jax.experimental.pallas import tpu as pltpu
from jax.sharding import PartitionSpec as P

TILE = 128
GROUP = 64
ROWS_MIN = 16
BUILD_UNROLL = 32
APPLY_UNROLL = 32
HOT = jnp.float8_e4m3fn
HOT_EXTRA = 32
EXTRA = 16
PIECES = 4
CORES = 2
MESH_ID = pl.DeviceIdType.MESH
VMEM_SPEC = pl.BlockSpec(memory_space=pltpu.VMEM)


def order_kernel(count_ref, rows_ref, cols_ref, order_ref):
    slots = rows_ref.shape[-1]
    places = order_ref.shape[-1]
    bins = ROWS_MIN * ((places - slots + ROWS_MIN - 1) // ROWS_MIN)
    bf16, f32 = jnp.bfloat16, jnp.float32

    def iota(shape, dim):
        return lax.broadcasted_iota(jnp.int32, shape, dim)

    def hot(mask):
        return jnp.where(mask, 1.0, 0.0).astype(bf16)

    def mul(x, y):
        return jnp.dot(x.astype(bf16), y.astype(bf16), preferred_element_type=f32)

    slot = iota((1, slots), 1)
    alive = slot < count_ref[0]
    rows = jnp.where(alive, rows_ref[...], -1)
    cols = jnp.where(alive, cols_ref[...], 0)
    belongs = rows == iota((bins, slots), 0)
    ranks = mul(hot(belongs), hot(iota((slots, slots), 0) <= iota((slots, slots), 1)))
    totals = jnp.broadcast_to(ranks[:, slots - 1 :], (bins, TILE)).astype(jnp.int32)
    pairs = (totals + 1) // 2
    before = hot(iota((bins, bins), 1) < iota((bins, bins), 0))
    offsets = 2.0 * (
        32.0 * mul(before, (pairs // 32).astype(f32)) + mul(before, (pairs % 32).astype(f32))
    )
    spots = jnp.where(belongs, ranks - 1.0 + offsets[:, :1], 0.0)
    spot = jnp.where(alive, jnp.sum(spots, axis=0, keepdims=True), -1.0)
    spot = jnp.broadcast_to(spot, (TILE, slots)).T.astype(jnp.int32)
    facts = [slot // 32, slot % 32, jnp.where(alive, 1, 0), rows, cols]
    facts = jnp.concatenate(
        [fact.astype(f32) for fact in facts] + [jnp.zeros((EXTRA - len(facts), slots), f32)], axis=0
    )
    for block in range(places // TILE):
        taken = hot(spot == iota((slots, TILE), 1) + block * TILE)
        found = mul(facts, taken).astype(jnp.int32)
        place = 32 * found[0:1] + found[1:2] + found[2:3] - 1
        order_ref[:, block * TILE : (block + 1) * TILE] = jnp.concatenate(
            [place, found[3:5], jnp.zeros((5, TILE), jnp.int32)], axis=0
        )
    end = jnp.sum(2.0 * pairs.astype(f32), axis=0, keepdims=True).astype(jnp.int32)
    order_ref[3:4, 0:TILE] = end


def turns_of(order_ref, unroll):
    first = pl.program_id(0) * GROUP
    left = jnp.clip(order_ref[3, 0] - first, 0, GROUP)
    return first, (left + unroll - 1) // unroll


def build_kernel(order_ref, dst_ref, src_ref, store_ref, degree_ref, degree_acc):
    @pl.when(pl.program_id(0) == 0)
    def _():
        degree_acc[...] = jnp.zeros_like(degree_acc)

    first, turns = turns_of(order_ref, BUILD_UNROLL)
    cells = lax.broadcasted_iota(jnp.int32, (TILE, TILE), 0)

    def visit(turn, carry):
        for pair in range(BUILD_UNROLL // 2):
            counts = []
            base = turn * BUILD_UNROLL + 2 * pair
            for side in range(2):
                slot = order_ref[0, first + base + side]
                safe = jnp.maximum(slot, 0)
                dst = jnp.where(slot >= 0, dst_ref[pl.ds(safe, 1), :], -1)
                src = src_ref[pl.ds(safe, 1), :]
                dst_hot = jnp.where(dst == cells, 1.0, 0.0).astype(HOT)
                src_hot = jnp.where(src == cells, 1.0, 0.0).astype(HOT)
                valid = jnp.broadcast_to(jnp.where(src >= 0, 1.0, 0.0), (HOT_EXTRA, TILE))
                left = jnp.concatenate([src_hot, valid.astype(HOT)], axis=0)
                both = lax.dot_general(
                    left, dst_hot, (((1,), (1,)), ((), ())), preferred_element_type=jnp.float32
                )
                store_ref[turn * (BUILD_UNROLL // 2) + pair, side * TILE : (side + 1) * TILE] = both[
                    :TILE
                ].astype(jnp.bfloat16)
                counts.append(both[TILE : TILE + 8])
            degree_acc[order_ref[1, first + base]] += counts[0] + counts[1]
        return carry

    lax.fori_loop(0, turns, visit, 0)

    @pl.when(pl.program_id(0) == pl.num_programs(0) - 1)
    def _():
        degree_ref[...] = degree_acc[:, 0, :]


def apply_kernel(order_ref, store_ref, source_ref, out_ref, acc):
    @pl.when(pl.program_id(0) == 0)
    def _():
        acc[...] = jnp.zeros_like(acc)

    first, turns = turns_of(order_ref, APPLY_UNROLL)

    def visit(turn, carry):
        for pair in range(APPLY_UNROLL // 2):
            base = first + turn * APPLY_UNROLL + 2 * pair
            sources = jnp.concatenate(
                [source_ref[order_ref[2, base]], source_ref[order_ref[2, base + 1]]], axis=1
            )
            acc[order_ref[1, base]] += jnp.dot(
                sources,
                store_ref[turn * (APPLY_UNROLL // 2) + pair],
                preferred_element_type=jnp.float32,
            )
        return carry

    lax.fori_loop(0, turns, visit, 0)

    @pl.when(pl.program_id(0) == pl.num_programs(0) - 1)
    def _():
        out_ref[...] = acc[...].astype(jnp.bfloat16)


def greet(targets):
    barrier = pltpu.get_barrier_semaphore()
    for target in targets:
        pl.semaphore_signal(barrier, inc=1, device_id=target, device_id_type=MESH_ID)
    pl.semaphore_wait(barrier, len(targets))


def row_peers(n_row):
    row, col = lax.axis_index("row"), lax.axis_index("col")
    return [(lax.rem(row + d, n_row), col) for d in range(1, n_row)]


def sibling_peers(n_col):
    row, col = lax.axis_index("row"), lax.axis_index("col")
    return [(row, lax.rem(col + CORES * d, n_col)) for d in range(1, n_col // CORES)]


def send(src, dst, send_sem, recv_sem, target):
    copy = pltpu.make_async_remote_copy(
        src_ref=src,
        dst_ref=dst,
        send_sem=send_sem,
        recv_sem=recv_sem,
        device_id=target,
        device_id_type=MESH_ID,
    )
    copy.start()
    return copy


def spread_rows(gathered_ref, start, size, sems, n_row, piece):
    send_sem, recv_sem = sems
    copies = []
    for d, target in enumerate(row_peers(n_row)):
        place = gathered_ref.at[pl.ds(start, size)]
        copies.append(send(place, place, send_sem.at[piece, d], recv_sem.at[piece, d], target))
    return copies


def start_kernel(
    n_row, n_col, part_ref, features_ref, gathered_ref, root_ref, taken, deg_send, deg_recv, row_send, row_recv
):
    row, col = lax.axis_index("row"), lax.axis_index("col")
    own = root_ref.shape[0]
    col_targets = [(row, lax.rem(col + d, n_col)) for d in range(1, n_col)]
    greet(col_targets + row_peers(n_row))
    copies = []
    for d, target in enumerate(col_targets):
        copies.append(
            send(
                part_ref.at[pl.ds(target[1] * own, own)],
                taken.at[d],
                deg_send.at[d],
                deg_recv.at[d],
                target,
            )
        )
    degree = part_ref[pl.ds(pl.multiple_of(col * own, own), own), :]
    for d, copy in enumerate(copies):
        copy.wait_recv()
        degree = degree + taken[d]
    root = lax.rsqrt(1.0 + degree)
    root_ref[...] = root
    size = own // PIECES
    for piece in range(PIECES):
        for tile in range(piece * size, (piece + 1) * size):
            block = features_ref[tile * TILE : (tile + 1) * TILE, :].astype(jnp.float32).T
            gathered_ref[row * own + tile] = (block * root[tile : tile + 1, :]).astype(jnp.bfloat16)
        copies += spread_rows(
            gathered_ref, row * own + piece * size, size, (row_send, row_recv), n_row, piece
        )
    for copy in copies[n_col - 1 :]:
        copy.wait_recv()
    for copy in copies:
        copy.wait_send()


def sum_kernel(n_row, n_col, spread, part_ref, root_ref, *refs):
    if spread:
        hop_ref, gathered_ref, near, staged, far, *sems = refs
        near_send, near_recv, far_send, far_recv, row_send, row_recv = sems
    else:
        hop_ref, near, staged, far, near_send, near_recv, far_send, far_recv = refs
    row, col = lax.axis_index("row"), lax.axis_index("col")
    core = lax.rem(col, CORES)
    chip = col // CORES
    n_chip = n_col // CORES
    partner = (row, chip * CORES + 1 - core)
    siblings = sibling_peers(n_col)
    greet([partner] + siblings + (row_peers(n_row) if spread else []))
    own = root_ref.shape[0]
    size = own // PIECES
    near_copies = {}
    for piece in range(PIECES):
        for d in list(range(1, n_chip)) + [0]:
            other = lax.rem(chip + d, n_chip)
            start = (other * CORES + 1 - core) * own + piece * size
            near_copies[piece, d] = send(
                part_ref.at[pl.ds(start, size)],
                near.at[piece, d],
                near_send.at[piece, d],
                near_recv.at[piece, d],
                partner,
            )
    far_copies = {}
    for piece in range(PIECES):
        for d in range(1, n_chip):
            other = lax.rem(chip + d, n_chip)
            near_copies[piece, d].wait_recv()
            start = (other * CORES + core) * own + piece * size
            staged[piece, d - 1] = (
                part_ref[pl.ds(start, size)].astype(jnp.float32)
                + near[piece, d].astype(jnp.float32)
            ).astype(jnp.bfloat16)
            far_copies[piece, d] = send(
                staged.at[piece, d - 1],
                far.at[piece, d - 1],
                far_send.at[piece, d - 1],
                far_recv.at[piece, d - 1],
                siblings[d - 1],
            )
    row_copies = []
    for piece in range(PIECES):
        near_copies[piece, 0].wait_recv()
        start = (chip * CORES + core) * own + piece * size
        total = part_ref[pl.ds(start, size)].astype(jnp.float32) + near[piece, 0].astype(
            jnp.float32
        )
        for d in range(1, n_chip):
            far_copies[piece, d].wait_recv()
            total = total + far[piece, d - 1].astype(jnp.float32)
        roots = [root_ref[piece * size + tile : piece * size + tile + 1, :] for tile in range(size)]
        if spread:
            for tile in range(size):
                gathered_ref[row * own + piece * size + tile] = (
                    total[tile] * (roots[tile] * roots[tile])
                ).astype(jnp.bfloat16)
            row_copies += spread_rows(
                gathered_ref, row * own + piece * size, size, (row_send, row_recv), n_row, piece
            )
        for tile in range(size):
            place = (piece * size + tile) * TILE
            hop_ref[place : place + TILE, :] = (total[tile] * roots[tile]).T.astype(jnp.bfloat16)
    for copy in row_copies:
        copy.wait_recv()
    for copy in list(near_copies.values()) + list(far_copies.values()) + row_copies:
        copy.wait_send()


def sems(*shape):
    return pltpu.SemaphoreType.DMA(shape)


def comm_params(ident):
    return pltpu.CompilerParams(
        collective_id=ident, has_side_effects=True, vmem_limit_bytes=48 * 2**20
    )


def local(features, tile_rows, tile_cols, edge_lists, tile_counts):
    node_count, feat_width = features.shape
    n_row, n_col = lax.axis_size("row"), lax.axis_size("col")
    own = node_count // TILE
    block_tiles = own * n_col
    source_tiles = own * n_row
    slots = tile_rows.shape[-1]
    bf16, f32 = jnp.bfloat16, jnp.float32
    places = -(-(slots + block_tiles) // TILE) * TILE

    order = pl.pallas_call(
        order_kernel,
        out_shape=jax.ShapeDtypeStruct((8, places), jnp.int32),
        in_specs=[pl.BlockSpec(memory_space=pltpu.SMEM), VMEM_SPEC, VMEM_SPEC],
        out_specs=VMEM_SPEC,
        compiler_params=pltpu.CompilerParams(vmem_limit_bytes=48 * 2**20),
        name="order",
    )(tile_counts[0], tile_rows[0], tile_cols[0])

    def last_live(turn, order_ref):
        return jnp.minimum(turn, (jnp.maximum(order_ref[3, 0], 1) - 1) // GROUP)

    store, degree = pl.pallas_call(
        build_kernel,
        grid_spec=pltpu.PrefetchScalarGridSpec(
            num_scalar_prefetch=1,
            grid=(places // GROUP,),
            in_specs=[
                pl.BlockSpec((None, None, None, slots, TILE), lambda i, o, side=side: (side, 0, 0, 0, 0))
                for side in range(2)
            ],
            out_specs=[
                pl.BlockSpec((GROUP // 2, 2 * TILE, TILE), lambda i, o: (last_live(i, o), 0, 0)),
                pl.BlockSpec((block_tiles, TILE), lambda i, o: (0, 0)),
            ],
            scratch_shapes=[pltpu.VMEM((block_tiles, 8, TILE), f32)],
        ),
        out_shape=[
            jax.ShapeDtypeStruct((places // 2, 2 * TILE, TILE), bf16),
            jax.ShapeDtypeStruct((block_tiles, TILE), f32),
        ],
        name="build",
    )(order, edge_lists, edge_lists)

    gathered_type = jax.ShapeDtypeStruct((source_tiles, feat_width, TILE), bf16)
    gathered, root = pl.pallas_call(
        functools.partial(start_kernel, n_row, n_col),
        out_shape=[gathered_type, jax.ShapeDtypeStruct((own, TILE), f32)],
        in_specs=[VMEM_SPEC] * 2,
        out_specs=[VMEM_SPEC] * 2,
        scratch_shapes=[
            pltpu.VMEM((n_col - 1, own, TILE), f32),
            sems(n_col - 1),
            sems(n_col - 1),
            sems(PIECES, n_row - 1),
            sems(PIECES, n_row - 1),
        ],
        compiler_params=comm_params(0),
        name="start",
    )(degree, features)

    def apply(sources):
        return pl.pallas_call(
            apply_kernel,
            grid_spec=pltpu.PrefetchScalarGridSpec(
                num_scalar_prefetch=1,
                grid=(places // GROUP,),
                in_specs=[
                    pl.BlockSpec((GROUP // 2, 2 * TILE, TILE), lambda i, o: (last_live(i, o), 0, 0)),
                    pl.BlockSpec((source_tiles, feat_width, TILE), lambda i, o: (0, 0, 0)),
                ],
                out_specs=pl.BlockSpec((block_tiles, feat_width, TILE), lambda i, o: (0, 0, 0)),
                scratch_shapes=[pltpu.VMEM((block_tiles, feat_width, TILE), f32)],
            ),
            out_shape=jax.ShapeDtypeStruct((block_tiles, feat_width, TILE), bf16),
            compiler_params=pltpu.CompilerParams(vmem_limit_bytes=48 * 2**20),
            name="apply",
        )(order, store, sources)

    def collect(part, spread):
        n_chip = n_col // CORES
        size = own // PIECES
        outs = [jax.ShapeDtypeStruct((node_count, feat_width), bf16)]
        semaphores = [sems(PIECES, n_chip)] * 2 + [sems(PIECES, n_chip - 1)] * 2
        if spread:
            outs.append(gathered_type)
            semaphores += [sems(PIECES, n_row - 1)] * 2
        return pl.pallas_call(
            functools.partial(sum_kernel, n_row, n_col, spread),
            out_shape=outs,
            in_specs=[VMEM_SPEC] * 2,
            out_specs=[VMEM_SPEC] * len(outs),
            scratch_shapes=[
                pltpu.VMEM((PIECES, n_chip, size, feat_width, TILE), bf16),
                pltpu.VMEM((PIECES, n_chip - 1, size, feat_width, TILE), bf16),
                pltpu.VMEM((PIECES, n_chip - 1, size, feat_width, TILE), bf16),
            ]
            + semaphores,
            compiler_params=comm_params(1 if spread else 2),
            name="spread" if spread else "finish",
        )(part, root)

    hop_one, gathered = collect(apply(gathered), True)
    (hop_two,) = collect(apply(gathered), False)
    return (hop_one, hop_two)


def solution(mesh):
    placed = (
        P(("row", "col"), None),
        P("row", "col", None),
        P("row", "col", None),
        P(None, "row", "col", None, None),
        P("row", "col"),
    )
    return jax.shard_map(
        local,
        mesh=mesh,
        in_specs=placed,
        out_specs=(P(("row", "col"), None), P(("row", "col"), None)),
        check_vma=False,
    )
```

```python
import functools

import jax
import jax.numpy as jnp
from jax import lax
from jax.experimental import pallas as pl
from jax.experimental.pallas import tpu as pltpu
from jax.sharding import PartitionSpec as P

TILE = 128
GROUP = 128
ROWS_MIN = 16
BUILD_UNROLL = 32
APPLY_UNROLL = 32
HOT = jnp.float8_e4m3fn
HOT_EXTRA = 32
EXTRA = 16
PIECES = 4
CORES = 2
MESH_ID = pl.DeviceIdType.MESH
VMEM_SPEC = pl.BlockSpec(memory_space=pltpu.VMEM)


def order_kernel(count_ref, rows_ref, cols_ref, order_ref):
    slots = rows_ref.shape[-1]
    places = order_ref.shape[-1]
    bins = ROWS_MIN * ((places - slots + ROWS_MIN - 1) // ROWS_MIN)
    bf16, f32 = jnp.bfloat16, jnp.float32

    def iota(shape, dim):
        return lax.broadcasted_iota(jnp.int32, shape, dim)

    def hot(mask):
        return jnp.where(mask, 1.0, 0.0).astype(bf16)

    def mul(x, y):
        return jnp.dot(x.astype(bf16), y.astype(bf16), preferred_element_type=f32)

    slot = iota((1, slots), 1)
    alive = slot < count_ref[0]
    rows = jnp.where(alive, rows_ref[...], -1)
    cols = jnp.where(alive, cols_ref[...], 0)
    belongs = rows == iota((bins, slots), 0)
    ranks = mul(hot(belongs), hot(iota((slots, slots), 0) <= iota((slots, slots), 1)))
    totals = jnp.broadcast_to(ranks[:, slots - 1 :], (bins, TILE)).astype(jnp.int32)
    pairs = (totals + 1) // 2
    before = hot(iota((bins, bins), 1) < iota((bins, bins), 0))
    offsets = 2.0 * (
        32.0 * mul(before, (pairs // 32).astype(f32)) + mul(before, (pairs % 32).astype(f32))
    )
    spots = jnp.where(belongs, ranks - 1.0 + offsets[:, :1], 0.0)
    spot = jnp.where(alive, jnp.sum(spots, axis=0, keepdims=True), -1.0)
    spot = jnp.broadcast_to(spot, (TILE, slots)).T.astype(jnp.int32)
    facts = [slot // 32, slot % 32, jnp.where(alive, 1, 0), rows, cols]
    facts = jnp.concatenate(
        [fact.astype(f32) for fact in facts] + [jnp.zeros((EXTRA - len(facts), slots), f32)], axis=0
    )
    for block in range(places // TILE):
        taken = hot(spot == iota((slots, TILE), 1) + block * TILE)
        found = mul(facts, taken).astype(jnp.int32)
        place = 32 * found[0:1] + found[1:2] + found[2:3] - 1
        order_ref[:, block * TILE : (block + 1) * TILE] = jnp.concatenate(
            [place, found[3:5], jnp.zeros((5, TILE), jnp.int32)], axis=0
        )
    end = jnp.sum(2.0 * pairs.astype(f32), axis=0, keepdims=True).astype(jnp.int32)
    order_ref[3:4, 0:TILE] = end


def turns_of(order_ref, unroll):
    first = pl.program_id(0) * GROUP
    left = jnp.clip(order_ref[3, 0] - first, 0, GROUP)
    return first, (left + unroll - 1) // unroll


def build_kernel(order_ref, dst_ref, src_ref, store_ref, degree_ref, degree_acc):
    @pl.when(pl.program_id(0) == 0)
    def _():
        degree_acc[...] = jnp.zeros_like(degree_acc)

    first, turns = turns_of(order_ref, BUILD_UNROLL)
    cells = lax.broadcasted_iota(jnp.int32, (TILE, TILE), 0)

    def visit(turn, carry):
        for pair in range(BUILD_UNROLL // 2):
            counts = []
            base = turn * BUILD_UNROLL + 2 * pair
            for side in range(2):
                slot = order_ref[0, first + base + side]
                safe = jnp.maximum(slot, 0)
                dst = jnp.where(slot >= 0, dst_ref[pl.ds(safe, 1), :], -1)
                src = src_ref[pl.ds(safe, 1), :]
                dst_hot = jnp.where(dst == cells, 1.0, 0.0).astype(HOT)
                src_hot = jnp.where(src == cells, 1.0, 0.0).astype(HOT)
                valid = jnp.broadcast_to(jnp.where(src >= 0, 1.0, 0.0), (HOT_EXTRA, TILE))
                left = jnp.concatenate([src_hot, valid.astype(HOT)], axis=0)
                both = lax.dot_general(
                    left, dst_hot, (((1,), (1,)), ((), ())), preferred_element_type=jnp.float32
                )
                store_ref[turn * (BUILD_UNROLL // 2) + pair, side * TILE : (side + 1) * TILE] = both[
                    :TILE
                ].astype(jnp.bfloat16)
                counts.append(both[TILE : TILE + 8])
            degree_acc[order_ref[1, first + base]] += counts[0] + counts[1]
        return carry

    lax.fori_loop(0, turns, visit, 0)

    @pl.when(pl.program_id(0) == pl.num_programs(0) - 1)
    def _():
        degree_ref[...] = degree_acc[:, 0, :]


def apply_kernel(order_ref, store_ref, source_ref, out_ref, acc):
    @pl.when(pl.program_id(0) == 0)
    def _():
        acc[...] = jnp.zeros_like(acc)

    first, turns = turns_of(order_ref, APPLY_UNROLL)

    def visit(turn, carry):
        for pair in range(APPLY_UNROLL // 2):
            base = first + turn * APPLY_UNROLL + 2 * pair
            sources = jnp.concatenate(
                [source_ref[order_ref[2, base]], source_ref[order_ref[2, base + 1]]], axis=1
            )
            acc[order_ref[1, base]] += jnp.dot(
                sources,
                store_ref[turn * (APPLY_UNROLL // 2) + pair],
                preferred_element_type=jnp.float32,
            )
        return carry

    lax.fori_loop(0, turns, visit, 0)

    @pl.when(pl.program_id(0) == pl.num_programs(0) - 1)
    def _():
        out_ref[...] = acc[...].astype(jnp.bfloat16)


def greet(targets):
    barrier = pltpu.get_barrier_semaphore()
    for target in targets:
        pl.semaphore_signal(barrier, inc=1, device_id=target, device_id_type=MESH_ID)
    pl.semaphore_wait(barrier, len(targets))


def row_peers(n_row):
    row, col = lax.axis_index("row"), lax.axis_index("col")
    return [(lax.rem(row + d, n_row), col) for d in range(1, n_row)]


def sibling_peers(n_col):
    row, col = lax.axis_index("row"), lax.axis_index("col")
    return [(row, lax.rem(col + CORES * d, n_col)) for d in range(1, n_col // CORES)]


def send(src, dst, send_sem, recv_sem, target):
    copy = pltpu.make_async_remote_copy(
        src_ref=src,
        dst_ref=dst,
        send_sem=send_sem,
        recv_sem=recv_sem,
        device_id=target,
        device_id_type=MESH_ID,
    )
    copy.start()
    return copy


def spread_rows(gathered_ref, start, size, sems, n_row, piece):
    send_sem, recv_sem = sems
    copies = []
    for d, target in enumerate(row_peers(n_row)):
        place = gathered_ref.at[pl.ds(start, size)]
        copies.append(send(place, place, send_sem.at[piece, d], recv_sem.at[piece, d], target))
    return copies


def start_kernel(
    n_row, n_col, part_ref, features_ref, gathered_ref, root_ref, taken, deg_send, deg_recv, row_send, row_recv
):
    row, col = lax.axis_index("row"), lax.axis_index("col")
    own = root_ref.shape[0]
    col_targets = [(row, lax.rem(col + d, n_col)) for d in range(1, n_col)]
    greet(col_targets + row_peers(n_row))
    copies = []
    for d, target in enumerate(col_targets):
        copies.append(
            send(
                part_ref.at[pl.ds(target[1] * own, own)],
                taken.at[d],
                deg_send.at[d],
                deg_recv.at[d],
                target,
            )
        )
    degree = part_ref[pl.ds(pl.multiple_of(col * own, own), own), :]
    for d, copy in enumerate(copies):
        copy.wait_recv()
        degree = degree + taken[d]
    root = lax.rsqrt(1.0 + degree)
    root_ref[...] = root
    size = own // PIECES
    for piece in range(PIECES):
        for tile in range(piece * size, (piece + 1) * size):
            block = features_ref[tile * TILE : (tile + 1) * TILE, :].astype(jnp.float32).T
            gathered_ref[row * own + tile] = (block * root[tile : tile + 1, :]).astype(jnp.bfloat16)
        copies += spread_rows(
            gathered_ref, row * own + piece * size, size, (row_send, row_recv), n_row, piece
        )
    for copy in copies[n_col - 1 :]:
        copy.wait_recv()
    for copy in copies:
        copy.wait_send()


def sum_kernel(n_row, n_col, spread, part_ref, root_ref, *refs):
    if spread:
        hop_ref, gathered_ref, near, staged, far, *sems = refs
        near_send, near_recv, far_send, far_recv, row_send, row_recv = sems
    else:
        hop_ref, near, staged, far, near_send, near_recv, far_send, far_recv = refs
    row, col = lax.axis_index("row"), lax.axis_index("col")
    core = lax.rem(col, CORES)
    chip = col // CORES
    n_chip = n_col // CORES
    partner = (row, chip * CORES + 1 - core)
    siblings = sibling_peers(n_col)
    greet([partner] + siblings + (row_peers(n_row) if spread else []))
    own = root_ref.shape[0]
    size = own // PIECES
    near_copies = {}
    for piece in range(PIECES):
        for d in list(range(1, n_chip)) + [0]:
            other = lax.rem(chip + d, n_chip)
            start = (other * CORES + 1 - core) * own + piece * size
            near_copies[piece, d] = send(
                part_ref.at[pl.ds(start, size)],
                near.at[piece, d],
                near_send.at[piece, d],
                near_recv.at[piece, d],
                partner,
            )
    far_copies = {}
    for piece in range(PIECES):
        for d in range(1, n_chip):
            other = lax.rem(chip + d, n_chip)
            near_copies[piece, d].wait_recv()
            start = (other * CORES + core) * own + piece * size
            staged[piece, d - 1] = (
                part_ref[pl.ds(start, size)].astype(jnp.float32)
                + near[piece, d].astype(jnp.float32)
            ).astype(jnp.bfloat16)
            far_copies[piece, d] = send(
                staged.at[piece, d - 1],
                far.at[piece, d - 1],
                far_send.at[piece, d - 1],
                far_recv.at[piece, d - 1],
                siblings[d - 1],
            )
    row_copies = []
    for piece in range(PIECES):
        near_copies[piece, 0].wait_recv()
        start = (chip * CORES + core) * own + piece * size
        total = part_ref[pl.ds(start, size)].astype(jnp.float32) + near[piece, 0].astype(
            jnp.float32
        )
        for d in range(1, n_chip):
            far_copies[piece, d].wait_recv()
            total = total + far[piece, d - 1].astype(jnp.float32)
        roots = [root_ref[piece * size + tile : piece * size + tile + 1, :] for tile in range(size)]
        if spread:
            for tile in range(size):
                gathered_ref[row * own + piece * size + tile] = (
                    total[tile] * (roots[tile] * roots[tile])
                ).astype(jnp.bfloat16)
            row_copies += spread_rows(
                gathered_ref, row * own + piece * size, size, (row_send, row_recv), n_row, piece
            )
        for tile in range(size):
            place = (piece * size + tile) * TILE
            hop_ref[place : place + TILE, :] = (total[tile] * roots[tile]).T.astype(jnp.bfloat16)
    for copy in row_copies:
        copy.wait_recv()
    for copy in list(near_copies.values()) + list(far_copies.values()) + row_copies:
        copy.wait_send()


def sems(*shape):
    return pltpu.SemaphoreType.DMA(shape)


def comm_params(ident):
    return pltpu.CompilerParams(
        collective_id=ident, has_side_effects=True, vmem_limit_bytes=48 * 2**20
    )


def local(features, tile_rows, tile_cols, edge_lists, tile_counts):
    node_count, feat_width = features.shape
    n_row, n_col = lax.axis_size("row"), lax.axis_size("col")
    own = node_count // TILE
    block_tiles = own * n_col
    source_tiles = own * n_row
    slots = tile_rows.shape[-1]
    bf16, f32 = jnp.bfloat16, jnp.float32
    places = -(-(slots + block_tiles) // TILE) * TILE

    order = pl.pallas_call(
        order_kernel,
        out_shape=jax.ShapeDtypeStruct((8, places), jnp.int32),
        in_specs=[pl.BlockSpec(memory_space=pltpu.SMEM), VMEM_SPEC, VMEM_SPEC],
        out_specs=VMEM_SPEC,
        compiler_params=pltpu.CompilerParams(vmem_limit_bytes=48 * 2**20),
        name="order",
    )(tile_counts[0], tile_rows[0], tile_cols[0])

    def last_live(turn, order_ref):
        return jnp.minimum(turn, (jnp.maximum(order_ref[3, 0], 1) - 1) // GROUP)

    store, degree = pl.pallas_call(
        build_kernel,
        grid_spec=pltpu.PrefetchScalarGridSpec(
            num_scalar_prefetch=1,
            grid=(places // GROUP,),
            in_specs=[
                pl.BlockSpec((None, None, None, slots, TILE), lambda i, o, side=side: (side, 0, 0, 0, 0))
                for side in range(2)
            ],
            out_specs=[
                pl.BlockSpec((GROUP // 2, 2 * TILE, TILE), lambda i, o: (last_live(i, o), 0, 0)),
                pl.BlockSpec((block_tiles, TILE), lambda i, o: (0, 0)),
            ],
            scratch_shapes=[pltpu.VMEM((block_tiles, 8, TILE), f32)],
        ),
        out_shape=[
            jax.ShapeDtypeStruct((places // 2, 2 * TILE, TILE), bf16),
            jax.ShapeDtypeStruct((block_tiles, TILE), f32),
        ],
        name="build",
    )(order, edge_lists, edge_lists)

    gathered_type = jax.ShapeDtypeStruct((source_tiles, feat_width, TILE), bf16)
    gathered, root = pl.pallas_call(
        functools.partial(start_kernel, n_row, n_col),
        out_shape=[gathered_type, jax.ShapeDtypeStruct((own, TILE), f32)],
        in_specs=[VMEM_SPEC] * 2,
        out_specs=[VMEM_SPEC] * 2,
        scratch_shapes=[
            pltpu.VMEM((n_col - 1, own, TILE), f32),
            sems(n_col - 1),
            sems(n_col - 1),
            sems(PIECES, n_row - 1),
            sems(PIECES, n_row - 1),
        ],
        compiler_params=comm_params(0),
        name="start",
    )(degree, features)

    def apply(sources):
        return pl.pallas_call(
            apply_kernel,
            grid_spec=pltpu.PrefetchScalarGridSpec(
                num_scalar_prefetch=1,
                grid=(places // GROUP,),
                in_specs=[
                    pl.BlockSpec((GROUP // 2, 2 * TILE, TILE), lambda i, o: (last_live(i, o), 0, 0)),
                    pl.BlockSpec((source_tiles, feat_width, TILE), lambda i, o: (0, 0, 0)),
                ],
                out_specs=pl.BlockSpec((block_tiles, feat_width, TILE), lambda i, o: (0, 0, 0)),
                scratch_shapes=[pltpu.VMEM((block_tiles, feat_width, TILE), f32)],
            ),
            out_shape=jax.ShapeDtypeStruct((block_tiles, feat_width, TILE), bf16),
            compiler_params=pltpu.CompilerParams(vmem_limit_bytes=48 * 2**20),
            name="apply",
        )(order, store, sources)

    def collect(part, spread):
        n_chip = n_col // CORES
        size = own // PIECES
        outs = [jax.ShapeDtypeStruct((node_count, feat_width), bf16)]
        semaphores = [sems(PIECES, n_chip)] * 2 + [sems(PIECES, n_chip - 1)] * 2
        if spread:
            outs.append(gathered_type)
            semaphores += [sems(PIECES, n_row - 1)] * 2
        return pl.pallas_call(
            functools.partial(sum_kernel, n_row, n_col, spread),
            out_shape=outs,
            in_specs=[VMEM_SPEC] * 2,
            out_specs=[VMEM_SPEC] * len(outs),
            scratch_shapes=[
                pltpu.VMEM((PIECES, n_chip, size, feat_width, TILE), bf16),
                pltpu.VMEM((PIECES, n_chip - 1, size, feat_width, TILE), bf16),
                pltpu.VMEM((PIECES, n_chip - 1, size, feat_width, TILE), bf16),
            ]
            + semaphores,
            compiler_params=comm_params(1 if spread else 2),
            name="spread" if spread else "finish",
        )(part, root)

    hop_one, gathered = collect(apply(gathered), True)
    (hop_two,) = collect(apply(gathered), False)
    return (hop_one, hop_two)


def solution(mesh):
    placed = (
        P(("row", "col"), None),
        P("row", "col", None),
        P("row", "col", None),
        P(None, "row", "col", None, None),
        P("row", "col"),
    )
    return jax.shard_map(
        local,
        mesh=mesh,
        in_specs=placed,
        out_specs=(P(("row", "col"), None), P(("row", "col"), None)),
        check_vma=False,
    )
```
